32 devices in a mesh: band: 4 (over x, core), grid: 8 (over z, y).
Axes of the slice: x: 2, y: 2, z: 4, core: 2. Of those that a mesh axis runs over, the one named last changes fastest.
Arguments:
- orbitals: bfloat16 [16384, 2048], P('grid', 'band'), may hold values from -6 to 6
- projectors: bfloat16 [64, 8, 128], replicated, may hold values from -0.5 to 0.5
- sphere_start: int32 [64], replicated, may hold values from 0 to 1920, as said below
- proj_count: int32 [64], replicated, may hold values from 1 to 8
- owner_slab: int32 [64], replicated, may hold values from 0 to 7, as said below
- correlation_coef: float32 [64, 8, 8], replicated, as said below
Outputs:
- rotated: bfloat16 [16384, 2048], P(('grid', 'band'))
The draws below stay inside these ranges and needn't reach their ends.
Inputs may be any that keep to these rules, and one draw needn't show every extreme that they name: `sphere_start`: a multiple of 128. `owner_slab`: every slab owns exactly 8 atoms. `correlation_coef`: each atom's matrix is symmetric positive definite.
All inputs are finite; a program needn't handle non-finite values.
Results may differ from the reference program's by a relative error of at most 0.0049.
Values may be sent and summed in bfloat16 or wider, within the bound.
No kernel may reach another device: no remote copies, remote signals or barrier semaphores. Data moves between devices by JAX's collectives and lax.ppermute only.
A program may use at most 128 MiB of HBM per device.

```python
import jax
import jax.numpy as jnp
from jax import lax

NB = 2048
SPH = 128
NPMAX = 8
A_SLAB = 8
G_SLAB = 2048
NG = 16384
NA = 64


def draw_owner_slab(key, part):
    order = jax.random.permutation(jax.random.fold_in(key, 11), NA)
    return (order // A_SLAB).astype(jnp.int32)


def draw_sphere_start(key, part):
    blocks = jax.random.randint(jax.random.fold_in(key, 12), (NA,), 0, G_SLAB // SPH)
    return (blocks * SPH).astype(jnp.int32)


def draw_correlation_coef(key, part):
    noise_key = jax.random.fold_in(key, 13)
    factor = jax.random.normal(noise_key, (NA, NPMAX, NPMAX), jnp.float32)
    square = jnp.einsum('aik,ajk->aij', factor, factor) / NPMAX
    square = square + 0.5 * jnp.eye(NPMAX, dtype=jnp.float32)[None, :, :]
    return (square / (NA * NPMAX)).astype(jnp.float32)


def touch_ends(values, stream_key, least, high):
    longest = values.shape.index(max(values.shape))
    spots = []
    for shift in (0, 1):
        where = [jax.random.randint(jax.random.fold_in(stream_key, axis), (), 0, length) for axis, length in enumerate(values.shape)]
        where[longest] = (where[longest] + shift) % values.shape[longest]
        spots.append(tuple(where))
    return values.at[spots[0]].set(least).at[spots[1]].set(high)


def shard_levels(stream_key, dims, pieces, low, high):
    loudness, own = 1.0, jax.random.fold_in(stream_key, 6)
    for position, blocks in pieces:
        heights = jnp.exp(jax.random.uniform(jax.random.fold_in(own, position), (blocks,), jnp.float32, low / len(pieces), high / len(pieces)))
        loudness = loudness * jnp.repeat(heights, dims[position] // blocks).reshape([-1 if axis == position else 1 for axis in range(len(dims))])
    return loudness


def centred(own_key, extent, width, bound, shards=(), kind=jnp.bfloat16):
    values = width * jax.random.normal(own_key, extent, jnp.float32)
    if shards:
        values = values * shard_levels(own_key, extent, shards, -0.22, 0.18)
    return jnp.clip(values, -bound, bound).astype(kind)


def setup_inputs(seed: int = 0) -> dict:
    key_of = jax.random.split(jax.random.key(seed), 7)
    orbitals = centred(key_of[0], (NG, NB), 1.0, 6.0, ((0, 8), (1, 4)))
    projectors = centred(key_of[1], (NA, NPMAX, SPH), SPH ** -0.5, 0.5)
    sphere_start = draw_sphere_start(jax.random.fold_in(key_of[6], 71), 0)
    proj_count = touch_ends(jax.random.randint(key_of[3], (NA,), 1, NPMAX + 1), jax.random.fold_in(key_of[3], 1), 1, NPMAX).astype(jnp.int32)
    owner_slab = draw_owner_slab(jax.random.fold_in(key_of[6], 71), 0)
    correlation_coef = draw_correlation_coef(jax.random.fold_in(key_of[6], 71), 0)
    return {"orbitals": orbitals, "projectors": projectors, "sphere_start": sphere_start, "proj_count": proj_count, "owner_slab": owner_slab, "correlation_coef": correlation_coef}


def inverse_factor(matrix):
    order = matrix.shape[0]
    if order <= 512 or order % 2 != 0:
        lower = jnp.linalg.cholesky(matrix)
        identity = jnp.eye(order, dtype=matrix.dtype)
        return lax.linalg.triangular_solve(lower, identity, left_side=True, lower=True)
    half = order // 2
    upper_inv = inverse_factor(matrix[:half, :half])
    below = jnp.dot(matrix[half:, :half], upper_inv.T, precision=lax.Precision.HIGHEST)
    schur = matrix[half:, half:] - jnp.dot(below, below.T, precision=lax.Precision.HIGHEST)
    lower_inv = inverse_factor(schur)
    corner = -jnp.dot(lower_inv, jnp.dot(below, upper_inv, precision=lax.Precision.HIGHEST), precision=lax.Precision.HIGHEST)
    top = jnp.concatenate([upper_inv, jnp.zeros((half, order - half), matrix.dtype)], axis=1)
    bottom = jnp.concatenate([corner, lower_inv], axis=1)
    return jnp.concatenate([top, bottom], axis=0)

def reference(orbitals, projectors, sphere_start, proj_count, owner_slab, correlation_coef):
    total_rows = orbitals.shape[0]
    bands = orbitals.shape[1]
    gram = jnp.dot(orbitals.T.astype(jnp.float32), orbitals.astype(jnp.float32), preferred_element_type=jnp.float32) * (1.0 / total_rows)
    starts = (owner_slab * G_SLAB + sphere_start).astype(jnp.int32)

    def one_atom(packed):
        weights, start, number, coefs = packed
        sphere_rows = lax.dynamic_slice_in_dim(orbitals, start, SPH, 0)
        correlations = jnp.dot(weights.astype(jnp.float32), sphere_rows.astype(jnp.float32), preferred_element_type=jnp.float32)
        active = jnp.arange(NPMAX) < number
        correlations = jnp.where(active[:, None], correlations, jnp.zeros_like(correlations))
        weighted = jnp.dot(coefs, correlations, precision=lax.Precision.HIGHEST)
        return (correlations, weighted)
    correlations, weighted = lax.map(one_atom, (projectors, starts, proj_count, correlation_coef))
    paw = jnp.dot(weighted.reshape(-1, bands).T, correlations.reshape(-1, bands), precision=lax.Precision.HIGHEST)
    metric = gram + paw
    inverse = inverse_factor(metric).astype(jnp.bfloat16)
    return jnp.dot(orbitals.astype(jnp.float32), inverse.T.astype(jnp.float32), preferred_element_type=jnp.float32).astype(jnp.bfloat16)
```

```python
import functools

import jax, jax.numpy as jnp
from jax import lax
from jax.experimental import pallas as pl
from jax.experimental.pallas import tpu as pltpu
from jax.sharding import PartitionSpec as P
f32,bf16=jnp.float32,jnp.bfloat16

def split(x):
    hi=x.astype(bf16)
    return hi,(x-hi.astype(f32)).astype(bf16)

def dotg(a,b,ca,cb):
    return lax.dot_general(a,b,(((ca,),(cb,)),((),())),preferred_element_type=f32)

def dot3(a,b,ca=1,cb=0):
    ah,al=split(a); bh,bl=split(b)
    return dotg(ah,bh,ca,cb)+(dotg(ah,bl,ca,cb)+dotg(al,bh,ca,cb))

def inverse_root(m):
    n=m.shape[0]
    lane=lax.broadcasted_iota(jnp.int32,(8,n),1)
    sub=lax.broadcasted_iota(jnp.int32,(8,n),0)
    def step(o,piv):
        k0=pl.multiple_of(o*8,8)
        rows=[jnp.broadcast_to(m[pl.ds(k0+k,1),:],(8,n)) for k in range(8)]
        idx=[jnp.full((8,n),k0+k,jnp.int32) for k in range(8)]
        s=[[None]*8 for _ in range(8)]
        for i in range(8):
            for k in range(i,8):
                s[i][k]=jnp.take_along_axis(rows[i],idx[k],axis=1)
        mult=[[None]*8 for _ in range(8)]
        inv=[None]*8
        for k in range(8):
            inv[k]=1.0/s[k][k]
            piv=jnp.where(lane==k0+k,s[k][k],piv)
            for j in range(k+1,8):
                mult[k][j]=s[k][j]*inv[k]
            for i in range(k+1,8):
                for j in range(i,8):
                    s[i][j]=s[i][j]-mult[k][i]*s[k][j]
            for j in range(k+1,8):
                rows[j]=rows[j]-mult[k][j]*rows[k]
        after=lane>k0+7
        r=[jnp.where(after,rows[k]*inv[k],jnp.where(lane==k0+k,-1.0,0.0)) for k in range(8)]
        for i in range(6,-1,-1):
            for k in range(7,i,-1):
                r[i]=r[i]-mult[i][k]*r[k]
        inside=(lane>=k0)&(lane<k0+8)
        for b in range(n//8):
            blk=m[b*8:b*8+8,:]
            new=jnp.where(inside,0.0,blk)
            for k in range(8):
                new=new-jnp.take_along_axis(blk,idx[k],axis=1)*r[k]
            m[b*8:b*8+8,:]=new
        own=-r[0]
        for k in range(1,8):
            own=jnp.where(sub==k,-r[k],own)
        m[pl.ds(k0,8),:]=own
        return piv
    return lax.fori_loop(0,n//8,step,jnp.ones((8,n),f32))

def invert_block(s,m,t):
    h=s.shape[0]//2
    m[...]=s[:h,:h]
    piv=inverse_root(m)
    t1=m[...]*lax.rsqrt(piv[0:1,:])
    low=dot3(s[h:,:h],t1)
    m[...]=s[h:,h:]-dot3(low,low,1,1)
    piv=inverse_root(m)
    t2=m[...]*lax.rsqrt(piv[0:1,:])
    t[:h,:h]=t1
    t[h:,h:]=t2
    t[h:,:h]=jnp.zeros((h,h),f32)
    t[:h,h:]=-dot3(t1,dot3(low,t2,0,0))

def factor_kernel(passes,a_ref,o_ref,y_ref,hi,lo,m,t,s,xb):
    nb=o_ref.shape[1]; B=256; n=nb//B; orow=o_ref.shape[0]
    off=0
    for p in range(n):
        K=p*B
        def upd(I,x):
            if p==0: return x
            rI=pl.ds(pl.multiple_of(I*B,B),B); rp=pl.ds(p*B,B)
            x=x-dotg(hi[rI,:K],hi[rp,:K],1,1)
            if passes==3:
                x=x-(dotg(hi[rI,:K],lo[rp,:K],1,1)+dotg(lo[rI,:K],hi[rp,:K],1,1))
            return x
        s[...]=upd(p,a_ref[off])
        invert_block(s[...],m,t)
        th,tl=split(t[...])
        def body(i,_):
            I=p+1+i
            x=upd(I,a_ref[off+1+i])
            xh,xl=split(x)
            r=dotg(xh,th,1,0)
            if passes==3:
                r=r+(dotg(xh,tl,1,0)+dotg(xl,th,1,0))
            rh=r.astype(bf16)
            hi[pl.ds(pl.multiple_of(I*B,B),B),p*B:(p+1)*B]=rh
            if passes==3:
                lo[pl.ds(pl.multiple_of(I*B,B),B),p*B:(p+1)*B]=(r-rh.astype(f32)).astype(bf16)
            return 0
        if p<n-1: lax.fori_loop(0,n-1-p,body,0)
        def obody(i,_):
            rr=pl.ds(pl.multiple_of(i*B,B),B)
            x=o_ref[rr,p*B:(p+1)*B].astype(f32)
            if p>0: x=x-dotg(y_ref[rr,:K],hi[p*B:(p+1)*B,:K],1,1)
            xh,xl=split(x)
            r=dotg(xh,th,1,0)+dotg(xl,th,1,0)
            y_ref[rr,p*B:(p+1)*B]=r.astype(bf16)
            return 0
        lax.fori_loop(0,orow//B,obody,0)
        off+=n-p

def factor_solve(a,o,passes=3,interpret=False):
    nb=o.shape[1]
    V=pl.BlockSpec(memory_space=pltpu.VMEM)
    return pl.pallas_call(functools.partial(factor_kernel,passes),
        out_shape=jax.ShapeDtypeStruct(o.shape,bf16),
        in_specs=[V,V],out_specs=V,
        scratch_shapes=[pltpu.VMEM((nb,nb),bf16),pltpu.VMEM((nb,nb) if passes==3 else (8,128),bf16),
            pltpu.VMEM((128,128),f32),pltpu.VMEM((256,256),f32),pltpu.VMEM((256,256),f32),pltpu.VMEM((256,256),f32)],
        compiler_params=pltpu.CompilerParams(vmem_limit_bytes=56*2**20),name="factor_solve",interpret=interpret)(a,o)


BLOCK = 256


def lower_blocks(count):
    return [(i, p) for p in range(count) for i in range(p, count)]


def metric_kernel(scale, ids, mine, weights, coefs, out, high, low, whigh, wlow):
    corr = jnp.dot(weights[...], mine[...], preferred_element_type=f32)
    weighted = dot3(coefs[...], corr) * (1.0 / scale)
    high[...], low[...] = split(corr)
    whigh[...], wlow[...] = split(weighted)

    def one(b, _):
        rows = pl.ds(pl.multiple_of(ids[b, 0] * BLOCK, BLOCK), BLOCK)
        cols = pl.ds(pl.multiple_of(ids[b, 1] * BLOCK, BLOCK), BLOCK)
        total = dotg(mine[:, rows], mine[:, cols], 0, 0)
        paw = dotg(whigh[:, rows], high[:, cols], 0, 0)
        paw = paw + dotg(whigh[:, rows], low[:, cols], 0, 0)
        paw = paw + dotg(wlow[:, rows], high[:, cols], 0, 0)
        out[b] = (total + paw) * scale
        return 0

    lax.fori_loop(0, out.shape[0], one, 0)


def metric_blocks(ids, mine, weights, coefs, scale):
    bands = mine.shape[1]
    terms = weights.shape[0]
    vmem = pl.BlockSpec(memory_space=pltpu.VMEM)
    return pl.pallas_call(
        functools.partial(metric_kernel, scale),
        out_shape=jax.ShapeDtypeStruct((ids.shape[0], BLOCK, BLOCK), f32),
        in_specs=[pl.BlockSpec(memory_space=pltpu.SMEM), vmem, vmem, vmem],
        out_specs=vmem,
        scratch_shapes=[pltpu.VMEM((terms, bands), bf16)] * 4,
        compiler_params=pltpu.CompilerParams(vmem_limit_bytes=56 * 2**20),
        name="metric_blocks",
    )(ids, mine, weights, coefs)


def atom_rows(projectors, sphere_start, proj_count, owner_slab, correlation_coef, first, height):
    slabs = lax.axis_size("grid")
    atoms, most, span = projectors.shape
    per_slab = atoms // slabs
    owned = owner_slab == lax.axis_index("grid")
    rank = jnp.cumsum(owned.astype(jnp.int32)) - 1
    pick = owned[None, :] & (rank[None, :] == jnp.arange(per_slab, dtype=jnp.int32)[:, None])

    def choose(values):
        shaped = pick.reshape(pick.shape + (1,) * (values.ndim - 1))
        return jnp.sum(jnp.where(shaped, values[None], jnp.zeros_like(values)[None]), axis=1, dtype=values.dtype)

    weights = choose(projectors)
    active = jnp.arange(most)[None, :] < choose(proj_count)[:, None]
    block = (choose(sphere_start) - first) // span
    spots = (block[:, None] == jnp.arange(height // span)[None, :])[:, None, :, None] & active[:, :, None, None]
    rows = jnp.where(spots, weights[:, :, None, :], jnp.zeros_like(weights)[:, :, None, :])
    coefs = choose(correlation_coef)
    same = jnp.eye(per_slab, dtype=bool)[:, None, :, None]
    square = jnp.where(same, coefs[:, :, None, :], 0.0)
    return rows.reshape(per_slab * most, height), square.reshape(per_slab * most, per_slab * most)


def shards(orbitals, projectors, sphere_start, proj_count, owner_slab, correlation_coef):
    total_rows = orbitals.shape[0] * lax.axis_size("grid")
    height = orbitals.shape[0] // lax.axis_size("band")
    first = lax.axis_index("band") * height
    weights, coefs = atom_rows(projectors, sphere_start, proj_count, owner_slab, correlation_coef, first, height)
    mine = lax.all_to_all(orbitals, "band", split_axis=0, concat_axis=1, tiled=True)
    ids = jnp.asarray(lower_blocks(mine.shape[1] // BLOCK), jnp.int32)
    metric = metric_blocks(ids, mine, weights, coefs, 1.0 / total_rows)
    metric = lax.psum(metric, ("band", "grid"))
    return factor_solve(metric, mine)


def solution(mesh):
    in_specs = (P("grid", "band"), P(), P(), P(), P(), P())
    out_specs = P(("grid", "band"), None)
    return jax.shard_map(shards, mesh=mesh, in_specs=in_specs, out_specs=out_specs, check_vma=False)
```

```python
import functools

import jax, jax.numpy as jnp
from jax import lax
from jax.experimental import pallas as pl
from jax.experimental.pallas import tpu as pltpu
from jax.sharding import PartitionSpec as P


f32,bf16=jnp.float32,jnp.bfloat16


def split(x):
    hi=x.astype(bf16)
    return hi,(x-hi.astype(f32)).astype(bf16)


def dotg(a,b,ca,cb):
    return lax.dot_general(a,b,(((ca,),(cb,)),((),())),preferred_element_type=f32)


def dot3(a,b,ca=1,cb=0):
    ah,al=split(a); bh,bl=split(b)
    return dotg(ah,bh,ca,cb)+(dotg(ah,bl,ca,cb)+dotg(al,bh,ca,cb))


def inverse_root(m, c, pv):
    n = m.shape[0]
    lane = lax.broadcasted_iota(jnp.int32, (8, n), 1)
    sub = lax.broadcasted_iota(jnp.int32, (8, n), 0)

    def step(o, piv):
        k0 = pl.multiple_of(o * 8, 8)
        block = m[pl.ds(k0, 8), :]
        for k in range(8):
            pv[k] = jnp.take_along_axis(block, jnp.full((8, n), k0 + k, jnp.int32), axis=1)
        rows = [jnp.broadcast_to(m[pl.ds(k0 + k, 1), :], (8, n)) for k in range(8)]
        s = [[None] * 8 for _ in range(8)]
        for k in range(8):
            for i in range(k + 1):
                s[i][k] = jnp.broadcast_to(pv[k, i : i + 1, :], (8, n))
        for k in range(8):
            c[k] = jnp.take_along_axis(m[...], jnp.full((n, n), k0 + k, jnp.int32), axis=1)
        mult = [[None] * 8 for _ in range(8)]
        inv = [None] * 8
        for k in range(8):
            inv[k] = 1.0 / s[k][k]
            piv = jnp.where(lane == k0 + k, s[k][k], piv)
            for j in range(k + 1, 8):
                mult[k][j] = s[k][j] * inv[k]
            for i in range(k + 1, 8):
                for j in range(i, 8):
                    s[i][j] = s[i][j] - mult[k][i] * s[k][j]
            for j in range(k + 1, 8):
                rows[j] = rows[j] - mult[k][j] * rows[k]
        after = lane > k0 + 7
        r = [jnp.where(after, rows[k] * inv[k], jnp.where(lane == k0 + k, -1.0, 0.0)) for k in range(8)]
        for i in range(6, -1, -1):
            for k in range(7, i, -1):
                r[i] = r[i] - mult[i][k] * r[k]
        inside = (lane >= k0) & (lane < k0 + 8)
        for b in range(0, n, 8):
            new = jnp.where(inside, 0.0, m[b : b + 8, :])
            for k in range(8):
                new = new - c[k, b : b + 8, :] * r[k]
            m[b : b + 8, :] = new
        own = -r[0]
        for k in range(1, 8):
            own = jnp.where(sub == k, -r[k], own)
        m[pl.ds(k0, 8), :] = own
        return piv

    return lax.fori_loop(0, n // 8, step, jnp.ones((8, n), f32))


def invert_block(s,m,t,c,pv):
    h=s.shape[0]//2
    m[...]=s[:h,:h]
    piv=inverse_root(m,c,pv)
    t1=m[...]*lax.rsqrt(piv[0:1,:])
    low=dot3(s[h:,:h],t1)
    m[...]=s[h:,h:]-dot3(low,low,1,1)
    piv=inverse_root(m,c,pv)
    t2=m[...]*lax.rsqrt(piv[0:1,:])
    t[:h,:h]=t1
    t[h:,h:]=t2
    t[h:,:h]=jnp.zeros((h,h),f32)
    t[:h,h:]=-dot3(t1,dot3(low,t2,0,0))


BLOCK = 256
GROUPS = (0, 1, 3)


def panel_groups(count):
    ends = GROUPS[1:] + (count,)
    return [range(a, min(b, count)) for a, b in zip(GROUPS, ends) if a < count]


def place_units(panels, count, devices):
    blocks = [(i, p) for p in panels for i in range(p, count)]
    size = -(-len(blocks) // devices)
    blocks += [blocks[-1]] * (size * devices - len(blocks))
    held = [blocks[d * size : (d + 1) * size] for d in range(devices)]
    where = {}
    for k, block in enumerate(blocks):
        where.setdefault(block, (k // size, k % size))
    return size, held, where


def fetch(band, pieces, buf, sem):
    copies = []
    for r, parts in enumerate(pieces):
        first = 0
        for part in parts:
            dst = buf.at[band ^ r, pl.ds(first, part.shape[0])]
            copies.append(pltpu.make_async_copy(part, dst, sem.at[len(copies)]))
            first += part.shape[0]
    for copy in copies:
        copy.start()
    for copy in copies:
        copy.wait()


def metric_kernel(scale, counts, with_rows, where, ids, weights, coefs, *refs):
    parts = sum(counts)
    flat, refs = refs[:parts], refs[parts:]
    pieces, at = [], 0
    for c in counts:
        pieces.append(flat[at : at + c])
        at += c
    outs, (mine, high, low, whigh, wlow, sem) = refs[:-6], refs[-6:]
    band = where[0]
    fetch(band, pieces, mine, sem)
    width = mine.shape[2]
    for j in range(mine.shape[0]):
        cols = slice(j * width, (j + 1) * width)
        corr = jnp.dot(weights[...], mine[j], preferred_element_type=f32)
        weighted = dot3(coefs[...], corr) * (1.0 / scale)
        high[:, cols], low[:, cols] = split(corr)
        whigh[:, cols], wlow[:, cols] = split(weighted)
    if with_rows:
        rows = outs[-1]
        outs = outs[:-1]
        height = rows.shape[0]
        for j in range(mine.shape[0]):
            own = pl.ds(pl.multiple_of(band * height, height), height)
            rows[:, j * width : (j + 1) * width] = mine[j, own, :]
    first = 0
    for out in outs:
        slabs, size, part, _ = out.shape

        def one(n, _, first=first, out=out, slabs=slabs, part=part):
            i, p = ids[first + n, 0], ids[first + n, 1]
            rows = pl.ds(pl.multiple_of(i * BLOCK, BLOCK), BLOCK)
            cols = pl.ds(pl.multiple_of(p * BLOCK, BLOCK), BLOCK)
            per = width // BLOCK
            left = mine[i // per, :, pl.ds(pl.multiple_of((i % per) * BLOCK, BLOCK), BLOCK)]
            right = mine[p // per, :, pl.ds(pl.multiple_of((p % per) * BLOCK, BLOCK), BLOCK)]
            total = dotg(left, right, 0, 0)
            paw = dotg(whigh[:, rows], high[:, cols], 0, 0)
            paw = paw + dotg(whigh[:, rows], low[:, cols], 0, 0)
            paw = paw + dotg(wlow[:, rows], high[:, cols], 0, 0)
            out[:, n] = ((total + paw) * scale).reshape(slabs, part, BLOCK)
            return 0

        lax.fori_loop(0, size, one, 0)
        first += size


def metric_units(band, ids, sizes, slabs, weights, coefs, pieces, scale, height):
    bands = sum(p[0].shape[1] for p in pieces)
    grid_rows = sum(part.shape[0] for part in pieces[0])
    terms = weights.shape[0]
    vmem = pl.BlockSpec(memory_space=pltpu.VMEM)
    smem = pl.BlockSpec(memory_space=pltpu.SMEM)
    hbm = pl.BlockSpec(memory_space=pl.ANY)
    flat = [part for p in pieces for part in p]
    outs = [jax.ShapeDtypeStruct((slabs, n, BLOCK // slabs, BLOCK), f32) for n in sizes]
    if height:
        outs.append(jax.ShapeDtypeStruct((height, bands), bf16))
    return pl.pallas_call(
        functools.partial(metric_kernel, scale, [len(p) for p in pieces], bool(height)),
        out_shape=outs,
        in_specs=[smem, smem, vmem, vmem] + [hbm] * len(flat),
        out_specs=[vmem] * len(outs),
        scratch_shapes=[pltpu.VMEM((len(pieces), grid_rows, bands // len(pieces)), bf16)]
        + [pltpu.VMEM((terms, bands), bf16)] * 4
        + [pltpu.SemaphoreType.DMA((len(flat),))],
        compiler_params=pltpu.CompilerParams(vmem_limit_bytes=56 * 2**20),
        cost_estimate=pl.CostEstimate(flops=sum(sizes) * 2 * grid_rows * BLOCK * BLOCK, bytes_accessed=2**23, transcendentals=0),
        name="metric_units",
    )(band, ids, weights, coefs, *flat)


def sum_kernel(got, out):
    total = got[0]
    for g in range(1, got.shape[0]):
        total = total + got[g]
    for g in range(out.shape[0]):
        out[g] = total


def sum_units(got):
    return pl.pallas_call(
        sum_kernel,
        out_shape=jax.ShapeDtypeStruct(got.shape, f32),
        in_specs=[pl.BlockSpec(memory_space=pltpu.VMEM)],
        out_specs=pl.BlockSpec(memory_space=pltpu.VMEM),
        name="sum_units",
    )(got)


def group_kernel(panels, npieces, earlier, last, where, spots, *refs):
    pieces = [[r] for r in refs[:npieces]]
    o_ref = refs[npieces]
    refs = refs[npieces + 1 :]
    olds = [refs[3 * q : 3 * q + 3] for q in range(earlier)]
    refs = refs[3 * earlier :]
    nout = 1 if last else 3
    outs, (buf, m, t, s, c, pv, sem) = refs[:nout], refs[nout : nout + 7]
    if last:
        y_out, (hi, lo) = outs[0], refs[nout + 7 :]
        base = panels[0] * BLOCK
        for q, (oh, ol, oy) in enumerate(olds):
            begin = sum(olds[k][2].shape[1] for k in range(q))
            y_out[:, begin : begin + oy.shape[1]] = oy[...]
    else:
        hi, lo, y_out = outs
        base = 0
    fetch(where[0], pieces, buf, sem)
    count = o_ref.shape[1] // BLOCK
    height = o_ref.shape[0]
    first = 0

    def block(k):
        return buf[spots[k, 0], :, spots[k, 1]].reshape(BLOCK, BLOCK)

    for step, p in enumerate(panels):
        K = step * BLOCK
        mine = slice(K, K + BLOCK)
        cp = slice(p * BLOCK, (p + 1) * BLOCK)
        stores = [(oh, ol, oy, oy.shape[1], 0) for oh, ol, oy in olds] + ([(hi, lo, y_out, K, base)] if K else [])

        def reduce_block(i, x):
            ri = pl.ds(pl.multiple_of(i * BLOCK, BLOCK), BLOCK)
            for h, l, _, k, _b in stores:
                x = x - dotg(h[ri, :k], h[cp, :k], 1, 1)
                x = x - (dotg(h[ri, :k], l[cp, :k], 1, 1) + dotg(l[ri, :k], h[cp, :k], 1, 1))
            return x

        s[...] = reduce_block(p, block(first))
        invert_block(s[...], m, t, c, pv)
        th, tl = split(t[...])

        def rows_below(n, _):
            i = p + 1 + n
            xh, xl = split(reduce_block(i, block(first + 1 + n)))
            r = dotg(xh, th, 1, 0) + (dotg(xh, tl, 1, 0) + dotg(xl, th, 1, 0))
            ri = pl.ds(pl.multiple_of(i * BLOCK, BLOCK), BLOCK)
            hi[ri, mine], lo[ri, mine] = split(r)
            return 0

        lax.fori_loop(0, count - 1 - p, rows_below, 0)

        def rows_orbital(n, _):
            ri = pl.ds(pl.multiple_of(n * BLOCK, BLOCK), BLOCK)
            x = o_ref[ri, cp].astype(f32)
            for h, _l, y, k, b in stores:
                x = x - dotg(y[ri, b : b + k], h[cp, :k], 1, 1)
            xh, xl = split(x)
            r = dotg(xh, th, 1, 0) + (dotg(xh, tl, 1, 0) + dotg(xl, th, 1, 0))
            y_out[ri, base + K : base + K + BLOCK] = r.astype(bf16)
            return 0

        lax.fori_loop(0, height // BLOCK, rows_orbital, 0)
        first += count - p


def solve_group(panels, band, spots, pieces, rows, olds):
    height, bands = rows.shape
    width = len(panels) * BLOCK
    last = panels[-1] + 1 == bands // BLOCK
    flat = [x for old in olds for x in old]
    vmem = pl.BlockSpec(memory_space=pltpu.VMEM)
    smem = pl.BlockSpec(memory_space=pltpu.SMEM)
    if last:
        outs = [jax.ShapeDtypeStruct((height, bands), bf16)]
        more = [pltpu.VMEM((bands, width), bf16)] * 2
    else:
        outs = [jax.ShapeDtypeStruct((bands, width), bf16)] * 2 + [jax.ShapeDtypeStruct((height, width), bf16)]
        more = []
    flops = len(panels) * 10 * 10**9
    return pl.pallas_call(
        functools.partial(group_kernel, list(panels), len(pieces), len(olds), last),
        out_shape=outs,
        in_specs=[smem, smem] + [pl.BlockSpec(memory_space=pl.ANY)] * len(pieces) + [vmem] * (1 + len(flat)),
        out_specs=[vmem] * len(outs),
        scratch_shapes=[
            pltpu.VMEM((len(pieces),) + pieces[0].shape, f32),
            pltpu.VMEM((BLOCK // 2, BLOCK // 2), f32),
            pltpu.VMEM((BLOCK, BLOCK), f32),
            pltpu.VMEM((BLOCK, BLOCK), f32),
            pltpu.VMEM((8, BLOCK // 2, BLOCK // 2), f32),
            pltpu.VMEM((8, 8, BLOCK // 2), f32),
            pltpu.SemaphoreType.DMA((len(pieces),)),
        ]
        + more,
        compiler_params=pltpu.CompilerParams(vmem_limit_bytes=56 * 2**20),
        cost_estimate=pl.CostEstimate(flops=flops, bytes_accessed=2**23, transcendentals=0),
        name="solve_group",
    )(band, spots, *pieces, rows, *flat)


def gather_bands(parts, size):
    held = {0: list(parts)}
    bit = size // 2
    while bit:
        swap = [(d, d ^ bit) for d in range(size)]
        for r in list(held):
            held[r | bit] = [lax.ppermute(x, "band", swap) for x in held[r]]
        bit //= 2
    return [held[r] for r in range(size)]


def atom_rows(projectors, sphere_start, proj_count, owner_slab, correlation_coef, height):
    slabs = lax.axis_size("grid")
    atoms, most, span = projectors.shape
    per_slab = atoms // slabs
    owned = owner_slab == lax.axis_index("grid")
    rank = jnp.cumsum(owned.astype(jnp.int32)) - 1
    pick = owned[None, :] & (rank[None, :] == jnp.arange(per_slab, dtype=jnp.int32)[:, None])

    def choose(values):
        shaped = pick.reshape(pick.shape + (1,) * (values.ndim - 1))
        return jnp.sum(jnp.where(shaped, values[None], jnp.zeros_like(values)[None]), axis=1, dtype=values.dtype)

    weights = choose(projectors)
    active = jnp.arange(most)[None, :] < choose(proj_count)[:, None]
    block = choose(sphere_start) // span
    spots = (block[:, None] == jnp.arange(height // span)[None, :])[:, None, :, None] & active[:, :, None, None]
    rows = jnp.where(spots, weights[:, :, None, :], jnp.zeros_like(weights)[:, :, None, :])
    coefs = choose(correlation_coef)
    same = jnp.eye(per_slab, dtype=bool)[:, None, :, None]
    square = jnp.where(same, coefs[:, :, None, :], 0.0)
    return rows.reshape(per_slab * most, height), square.reshape(per_slab * most, per_slab * most)


def shards(orbitals, projectors, sphere_start, proj_count, owner_slab, correlation_coef):
    slabs, devices = lax.axis_size("grid"), lax.axis_size("band")
    grid_rows, width = orbitals.shape
    scale = 1.0 / (grid_rows * slabs)
    height = grid_rows // devices
    count = width * devices // BLOCK
    band_index = lax.axis_index("band")
    band = band_index.reshape(1)
    half = grid_rows // 2
    pieces = gather_bands([orbitals[:half], orbitals[half:]], devices)
    pieces[0] = [orbitals]
    weights, coefs = atom_rows(projectors, sphere_start, proj_count, owner_slab, correlation_coef, grid_rows)

    groups = panel_groups(count)
    plans = [place_units(panels, count, devices) for panels in groups]
    tables = [jnp.asarray(held, jnp.int32)[band_index] for _, held, _ in plans]
    sizes = [size for size, _, _ in plans]
    lead, rows = metric_units(band, tables[0], sizes[:1], slabs, weights, coefs, pieces, scale, height)
    rest = metric_units(band, jnp.concatenate(tables[1:]), sizes[1:], slabs, weights, coefs, pieces, scale, 0)
    olds = []
    for panels, (_, _, where), units in zip(groups, plans, [lead] + list(rest)):
        got = lax.all_to_all(units, "grid", split_axis=0, concat_axis=0, tiled=True)
        part = sum_units(got)
        part = lax.all_to_all(part, "grid", split_axis=0, concat_axis=0, tiled=True)
        all_parts = [x[0] for x in gather_bands([part], devices)]
        runs = [list(panels)] if panels[-1] + 1 == count else [[p] for p in panels]
        for run in runs:
            order = [where[i, p] for p in run for i in range(p, count)]
            olds.append(solve_group(run, band, jnp.asarray(order, jnp.int32), all_parts, rows, olds))
    return olds[-1][0]


def solution(mesh):
    in_specs = (P("grid", "band"), P(), P(), P(), P(), P())
    out_specs = P(("grid", "band"), None)
    return jax.shard_map(shards, mesh=mesh, in_specs=in_specs, out_specs=out_specs, check_vma=False)
```

```python
import functools

import jax, jax.numpy as jnp
from jax import lax
from jax.experimental import pallas as pl
from jax.experimental.pallas import tpu as pltpu
from jax.sharding import PartitionSpec as P


f32,bf16=jnp.float32,jnp.bfloat16


def split(x):
    hi=x.astype(bf16)
    return hi,(x-hi.astype(f32)).astype(bf16)


def dotg(a,b,ca,cb):
    return lax.dot_general(a,b,(((ca,),(cb,)),((),())),preferred_element_type=f32)


def dot3(a,b,ca=1,cb=0):
    ah,al=split(a); bh,bl=split(b)
    return dotg(ah,bh,ca,cb)+(dotg(ah,bl,ca,cb)+dotg(al,bh,ca,cb))


def inverse_root(m, c, pv):
    n = m.shape[0]
    lane = lax.broadcasted_iota(jnp.int32, (8, n), 1)
    sub = lax.broadcasted_iota(jnp.int32, (8, n), 0)

    def step(o, piv):
        k0 = pl.multiple_of(o * 8, 8)
        block = m[pl.ds(k0, 8), :]
        for k in range(8):
            pv[k] = jnp.take_along_axis(block, jnp.full((8, n), k0 + k, jnp.int32), axis=1)
        rows = [jnp.broadcast_to(m[pl.ds(k0 + k, 1), :], (8, n)) for k in range(8)]
        s = [[None] * 8 for _ in range(8)]
        for k in range(8):
            for i in range(k + 1):
                s[i][k] = jnp.broadcast_to(pv[k, i : i + 1, :], (8, n))
        for k in range(8):
            c[k] = jnp.take_along_axis(m[...], jnp.full((n, n), k0 + k, jnp.int32), axis=1)
        mult = [[None] * 8 for _ in range(8)]
        inv = [None] * 8
        for k in range(8):
            inv[k] = 1.0 / s[k][k]
            piv = jnp.where(lane == k0 + k, s[k][k], piv)
            for j in range(k + 1, 8):
                mult[k][j] = s[k][j] * inv[k]
            for i in range(k + 1, 8):
                for j in range(i, 8):
                    s[i][j] = s[i][j] - mult[k][i] * s[k][j]
            for j in range(k + 1, 8):
                rows[j] = rows[j] - mult[k][j] * rows[k]
        after = lane > k0 + 7
        r = [jnp.where(after, rows[k] * inv[k], jnp.where(lane == k0 + k, -1.0, 0.0)) for k in range(8)]
        for i in range(6, -1, -1):
            for k in range(7, i, -1):
                r[i] = r[i] - mult[i][k] * r[k]
        inside = (lane >= k0) & (lane < k0 + 8)
        for b in range(0, n, 8):
            new = jnp.where(inside, 0.0, m[b : b + 8, :])
            for k in range(8):
                new = new - c[k, b : b + 8, :] * r[k]
            m[b : b + 8, :] = new
        own = -r[0]
        for k in range(1, 8):
            own = jnp.where(sub == k, -r[k], own)
        m[pl.ds(k0, 8), :] = own
        return piv

    return lax.fori_loop(0, n // 8, step, jnp.ones((8, n), f32))


def invert_block(s,m,t,c,pv):
    h=s.shape[0]//2
    m[...]=s[:h,:h]
    piv=inverse_root(m,c,pv)
    t1=m[...]*lax.rsqrt(piv[0:1,:])
    low=dot3(s[h:,:h],t1)
    m[...]=s[h:,h:]-dot3(low,low,1,1)
    piv=inverse_root(m,c,pv)
    t2=m[...]*lax.rsqrt(piv[0:1,:])
    t[:h,:h]=t1
    t[h:,h:]=t2
    t[h:,:h]=jnp.zeros((h,h),f32)
    t[:h,h:]=-dot3(t1,dot3(low,t2,0,0))


BLOCK = 256
GROUPS = (0, 1, 3)


def panel_groups(count):
    ends = GROUPS[1:] + (count,)
    return [range(a, min(b, count)) for a, b in zip(GROUPS, ends) if a < count]


def place_units(panels, count, devices):
    blocks = [(i, p) for p in panels for i in range(p, count)]
    size = -(-len(blocks) // devices)
    blocks += [blocks[-1]] * (size * devices - len(blocks))
    held = [blocks[d * size : (d + 1) * size] for d in range(devices)]
    where = {}
    for k, block in enumerate(blocks):
        where.setdefault(block, (k // size, k % size))
    return size, held, where


def fetch(band, pieces, buf, sem):
    copies = []
    for r, parts in enumerate(pieces):
        first = 0
        for part in parts:
            dst = buf.at[band ^ r, pl.ds(first, part.shape[0])]
            copies.append(pltpu.make_async_copy(part, dst, sem.at[len(copies)]))
            first += part.shape[0]
    for copy in copies:
        copy.start()
    for copy in copies:
        copy.wait()


def metric_kernel(scale, counts, with_rows, where, ids, weights, coefs, *refs):
    parts = sum(counts)
    flat, refs = refs[:parts], refs[parts:]
    pieces, at = [], 0
    for c in counts:
        pieces.append(flat[at : at + c])
        at += c
    outs, (mine, high, low, whigh, wlow, sem) = refs[:-6], refs[-6:]
    band = where[0]
    fetch(band, pieces, mine, sem)
    width = mine.shape[2]
    for j in range(mine.shape[0]):
        cols = slice(j * width, (j + 1) * width)
        corr = jnp.dot(weights[...], mine[j], preferred_element_type=f32)
        weighted = dot3(coefs[...], corr) * (1.0 / scale)
        high[:, cols], low[:, cols] = split(corr)
        whigh[:, cols], wlow[:, cols] = split(weighted)
    if with_rows:
        rows = outs[-1]
        outs = outs[:-1]
        height = rows.shape[0]
        for j in range(mine.shape[0]):
            own = pl.ds(pl.multiple_of(band * height, height), height)
            rows[:, j * width : (j + 1) * width] = mine[j, own, :]
    first = 0
    for out in outs:
        slabs, size, part, _ = out.shape

        def one(n, _, first=first, out=out, slabs=slabs, part=part):
            i, p = ids[first + n, 0], ids[first + n, 1]
            rows = pl.ds(pl.multiple_of(i * BLOCK, BLOCK), BLOCK)
            cols = pl.ds(pl.multiple_of(p * BLOCK, BLOCK), BLOCK)
            per = width // BLOCK
            left = mine[i // per, :, pl.ds(pl.multiple_of((i % per) * BLOCK, BLOCK), BLOCK)]
            right = mine[p // per, :, pl.ds(pl.multiple_of((p % per) * BLOCK, BLOCK), BLOCK)]
            total = dotg(left, right, 0, 0)
            paw = dotg(whigh[:, rows], high[:, cols], 0, 0)
            paw = paw + dotg(whigh[:, rows], low[:, cols], 0, 0)
            paw = paw + dotg(wlow[:, rows], high[:, cols], 0, 0)
            out[:, n] = ((total + paw) * scale).reshape(slabs, part, BLOCK)
            return 0

        lax.fori_loop(0, size, one, 0)
        first += size


def metric_units(band, ids, sizes, slabs, weights, coefs, pieces, scale, height):
    bands = sum(p[0].shape[1] for p in pieces)
    grid_rows = sum(part.shape[0] for part in pieces[0])
    terms = weights.shape[0]
    vmem = pl.BlockSpec(memory_space=pltpu.VMEM)
    smem = pl.BlockSpec(memory_space=pltpu.SMEM)
    hbm = pl.BlockSpec(memory_space=pl.ANY)
    flat = [part for p in pieces for part in p]
    outs = [jax.ShapeDtypeStruct((slabs, n, BLOCK // slabs, BLOCK), f32) for n in sizes]
    if height:
        outs.append(jax.ShapeDtypeStruct((height, bands), bf16))
    return pl.pallas_call(
        functools.partial(metric_kernel, scale, [len(p) for p in pieces], bool(height)),
        out_shape=outs,
        in_specs=[smem, smem, vmem, vmem] + [hbm] * len(flat),
        out_specs=[vmem] * len(outs),
        scratch_shapes=[pltpu.VMEM((len(pieces), grid_rows, bands // len(pieces)), bf16)]
        + [pltpu.VMEM((terms, bands), bf16)] * 4
        + [pltpu.SemaphoreType.DMA((len(flat),))],
        compiler_params=pltpu.CompilerParams(vmem_limit_bytes=28 * 2**20),
        cost_estimate=pl.CostEstimate(flops=sum(sizes) * 2 * grid_rows * BLOCK * BLOCK, bytes_accessed=2**23, transcendentals=0),
        name="metric_units",
    )(band, ids, weights, coefs, *flat)


def lead_kernel(scale, own, lead, weights, coefs, out, high, low, whigh, wlow):
    slabs, size, part, _ = out.shape
    corr = jnp.dot(weights[...], own[...], preferred_element_type=f32)
    whigh[...], wlow[...] = split(dot3(coefs[...], corr) * (1.0 / scale))
    high[...], low[...] = split(jnp.dot(weights[...], lead[...], preferred_element_type=f32))
    for n in range(size):
        rows = slice(n * BLOCK, (n + 1) * BLOCK)
        total = dotg(own[:, rows], lead[...], 0, 0)
        paw = dotg(whigh[:, rows], high[...], 0, 0)
        paw = paw + dotg(whigh[:, rows], low[...], 0, 0)
        paw = paw + dotg(wlow[:, rows], high[...], 0, 0)
        out[:, n] = ((total + paw) * scale).reshape(slabs, part, BLOCK)


def lead_units(slabs, weights, coefs, own, lead, scale):
    rows, width = own.shape
    terms = weights.shape[0]
    size = width // BLOCK
    vmem = pl.BlockSpec(memory_space=pltpu.VMEM)
    return pl.pallas_call(
        functools.partial(lead_kernel, scale),
        out_shape=jax.ShapeDtypeStruct((slabs, size, BLOCK // slabs, BLOCK), f32),
        in_specs=[vmem] * 4,
        out_specs=vmem,
        scratch_shapes=[pltpu.VMEM((terms, BLOCK), bf16)] * 2 + [pltpu.VMEM((terms, width), bf16)] * 2,
        compiler_params=pltpu.CompilerParams(vmem_limit_bytes=40 * 2**20),
        cost_estimate=pl.CostEstimate(flops=2 * rows * width * BLOCK, bytes_accessed=2**22, transcendentals=0),
        name="lead_units",
    )(own, lead, weights, coefs)


def spread_lead(value, index, size):
    held = jnp.where(index == 0, value, jnp.zeros_like(value))
    bit = size // 2
    while bit:
        pairs = [(d, d | bit) for d in range(0, size, 2 * bit)]
        got = lax.ppermute(held, "band", pairs)
        held = jnp.where(index & bit == 0, held, got)
        bit //= 2
    return held


def sum_kernel(got, out):
    total = got[0]
    for g in range(1, got.shape[0]):
        total = total + got[g]
    for g in range(out.shape[0]):
        out[g] = total


def sum_units(got):
    return pl.pallas_call(
        sum_kernel,
        out_shape=jax.ShapeDtypeStruct(got.shape, f32),
        in_specs=[pl.BlockSpec(memory_space=pltpu.VMEM)],
        out_specs=pl.BlockSpec(memory_space=pltpu.VMEM),
        name="sum_units",
    )(got)


def group_kernel(panels, npieces, earlier, last, where, spots, *refs):
    pieces = [[r] for r in refs[:npieces]]
    o_ref = refs[npieces]
    refs = refs[npieces + 1 :]
    olds = [refs[3 * q : 3 * q + 3] for q in range(earlier)]
    refs = refs[3 * earlier :]
    nout = 1 if last else 3
    outs, (buf, m, t, s, c, pv, sem) = refs[:nout], refs[nout : nout + 7]
    if last:
        y_out, (hi, lo) = outs[0], refs[nout + 7 :]
        base = panels[0] * BLOCK
        for q, (oh, ol, oy) in enumerate(olds):
            begin = sum(olds[k][2].shape[1] for k in range(q))
            y_out[:, begin : begin + oy.shape[1]] = oy[...]
    else:
        hi, lo, y_out = outs
        base = 0
    fetch(where[0], pieces, buf, sem)
    count = o_ref.shape[1] // BLOCK
    height = o_ref.shape[0]
    first = 0

    def block(k):
        return buf[spots[k, 0], :, spots[k, 1]].reshape(BLOCK, BLOCK)

    for step, p in enumerate(panels):
        K = step * BLOCK
        mine = slice(K, K + BLOCK)
        cp = slice(p * BLOCK, (p + 1) * BLOCK)
        stores = [(oh, ol, oy, oy.shape[1], 0) for oh, ol, oy in olds] + ([(hi, lo, y_out, K, base)] if K else [])

        def reduce_block(i, x):
            ri = pl.ds(pl.multiple_of(i * BLOCK, BLOCK), BLOCK)
            for h, l, _, k, _b in stores:
                x = x - dotg(h[ri, :k], h[cp, :k], 1, 1)
                x = x - (dotg(h[ri, :k], l[cp, :k], 1, 1) + dotg(l[ri, :k], h[cp, :k], 1, 1))
            return x

        s[...] = reduce_block(p, block(first))
        invert_block(s[...], m, t, c, pv)
        th, tl = split(t[...])

        def rows_below(n, _):
            i = p + 1 + n
            xh, xl = split(reduce_block(i, block(first + 1 + n)))
            r = dotg(xh, th, 1, 0) + (dotg(xh, tl, 1, 0) + dotg(xl, th, 1, 0))
            ri = pl.ds(pl.multiple_of(i * BLOCK, BLOCK), BLOCK)
            hi[ri, mine], lo[ri, mine] = split(r)
            return 0

        lax.fori_loop(0, count - 1 - p, rows_below, 0)

        def rows_orbital(n, _):
            ri = pl.ds(pl.multiple_of(n * BLOCK, BLOCK), BLOCK)
            x = o_ref[ri, cp].astype(f32)
            for h, _l, y, k, b in stores:
                x = x - dotg(y[ri, b : b + k], h[cp, :k], 1, 1)
            xh, xl = split(x)
            r = dotg(xh, th, 1, 0) + (dotg(xh, tl, 1, 0) + dotg(xl, th, 1, 0))
            y_out[ri, base + K : base + K + BLOCK] = r.astype(bf16)
            return 0

        lax.fori_loop(0, height // BLOCK, rows_orbital, 0)
        first += count - p


def solve_group(panels, band, spots, pieces, rows, olds):
    height, bands = rows.shape
    width = len(panels) * BLOCK
    last = panels[-1] + 1 == bands // BLOCK
    flat = [x for old in olds for x in old]
    vmem = pl.BlockSpec(memory_space=pltpu.VMEM)
    smem = pl.BlockSpec(memory_space=pltpu.SMEM)
    if last:
        outs = [jax.ShapeDtypeStruct((height, bands), bf16)]
        more = [pltpu.VMEM((bands, width), bf16)] * 2
    else:
        outs = [jax.ShapeDtypeStruct((bands, width), bf16)] * 2 + [jax.ShapeDtypeStruct((height, width), bf16)]
        more = []
    flops = len(panels) * 10 * 10**9
    return pl.pallas_call(
        functools.partial(group_kernel, list(panels), len(pieces), len(olds), last),
        out_shape=outs,
        in_specs=[smem, smem] + [pl.BlockSpec(memory_space=pl.ANY)] * len(pieces) + [vmem] * (1 + len(flat)),
        out_specs=[vmem] * len(outs),
        scratch_shapes=[
            pltpu.VMEM((len(pieces),) + pieces[0].shape, f32),
            pltpu.VMEM((BLOCK // 2, BLOCK // 2), f32),
            pltpu.VMEM((BLOCK, BLOCK), f32),
            pltpu.VMEM((BLOCK, BLOCK), f32),
            pltpu.VMEM((8, BLOCK // 2, BLOCK // 2), f32),
            pltpu.VMEM((8, 8, BLOCK // 2), f32),
            pltpu.SemaphoreType.DMA((len(pieces),)),
        ]
        + more,
        compiler_params=pltpu.CompilerParams(vmem_limit_bytes=36 * 2**20),
        cost_estimate=pl.CostEstimate(flops=flops, bytes_accessed=2**23, transcendentals=0),
        name="solve_group",
    )(band, spots, *pieces, rows, *flat)


def gather_bands(parts, size):
    held = {0: list(parts)}
    bit = size // 2
    while bit:
        swap = [(d, d ^ bit) for d in range(size)]
        for r in list(held):
            got = []
            for x in held[r]:
                got.append(lax.ppermute(x, "band", swap))
            held[r | bit] = got
        bit //= 2
    return [held[r] for r in range(size)]


def atom_rows(projectors, sphere_start, proj_count, owner_slab, correlation_coef, height):
    slabs = lax.axis_size("grid")
    atoms, most, span = projectors.shape
    per_slab = atoms // slabs
    owned = owner_slab == lax.axis_index("grid")
    rank = jnp.cumsum(owned.astype(jnp.int32)) - 1
    pick = owned[None, :] & (rank[None, :] == jnp.arange(per_slab, dtype=jnp.int32)[:, None])

    def choose(values):
        shaped = pick.reshape(pick.shape + (1,) * (values.ndim - 1))
        return jnp.sum(jnp.where(shaped, values[None], jnp.zeros_like(values)[None]), axis=1, dtype=values.dtype)

    weights = choose(projectors)
    active = jnp.arange(most)[None, :] < choose(proj_count)[:, None]
    block = choose(sphere_start) // span
    spots = (block[:, None] == jnp.arange(height // span)[None, :])[:, None, :, None] & active[:, :, None, None]
    rows = jnp.where(spots, weights[:, :, None, :], jnp.zeros_like(weights)[:, :, None, :])
    coefs = choose(correlation_coef)
    same = jnp.eye(per_slab, dtype=bool)[:, None, :, None]
    square = jnp.where(same, coefs[:, :, None, :], 0.0)
    return rows.reshape(per_slab * most, height), square.reshape(per_slab * most, per_slab * most)


def shards(orbitals, projectors, sphere_start, proj_count, owner_slab, correlation_coef):
    slabs, devices = lax.axis_size("grid"), lax.axis_size("band")
    grid_rows, width = orbitals.shape
    scale = 1.0 / (grid_rows * slabs)
    height = grid_rows // devices
    count = width * devices // BLOCK
    band_index = lax.axis_index("band")
    band = band_index.reshape(1)
    half = grid_rows // 2
    lead = spread_lead(orbitals[:, :BLOCK], band_index, devices)
    pieces = gather_bands([orbitals[:half], orbitals[half:]], devices)
    pieces[0] = [orbitals]
    weights, coefs = atom_rows(projectors, sphere_start, proj_count, owner_slab, correlation_coef, grid_rows)

    groups = panel_groups(count)
    plans = [place_units(panels, count, devices) for panels in groups]
    tables = [jnp.asarray(held, jnp.int32)[band_index] for _, held, _ in plans]
    assert plans[0][0] == width // BLOCK
    sizes = [size for size, _, _ in plans]
    first = lead_units(slabs, weights, coefs, orbitals, lead, scale)
    second, rows = metric_units(band, tables[1], sizes[1:2], slabs, weights, coefs, pieces, scale, height)
    ids = jnp.concatenate(tables[2:])
    rest = metric_units(band, ids, sizes[2:], slabs, weights, coefs, pieces, scale, 0)
    olds = []
    for panels, (_, _, where), units in zip(groups, plans, [first, second] + list(rest)):
        got = lax.all_to_all(units, "grid", split_axis=0, concat_axis=0, tiled=True)
        part = sum_units(got)
        part = lax.all_to_all(part, "grid", split_axis=0, concat_axis=0, tiled=True)
        all_parts = [x[0] for x in gather_bands([part], devices)]
        runs = [list(panels)] if panels[-1] + 1 == count else [[p] for p in panels]
        for run in runs:
            order = [where[i, p] for p in run for i in range(p, count)]
            olds.append(solve_group(run, band, jnp.asarray(order, jnp.int32), all_parts, rows, olds))
    return olds[-1][0]


def solution(mesh):
    in_specs = (P("grid", "band"), P(), P(), P(), P(), P())
    out_specs = P(("grid", "band"), None)
    return jax.shard_map(shards, mesh=mesh, in_specs=in_specs, out_specs=out_specs, check_vma=False)
```

```python
import functools

import jax, jax.numpy as jnp
from jax import lax
from jax.experimental import pallas as pl
from jax.experimental.pallas import tpu as pltpu
from jax.sharding import PartitionSpec as P


f32,bf16=jnp.float32,jnp.bfloat16


def split(x):
    hi=x.astype(bf16)
    return hi,(x-hi.astype(f32)).astype(bf16)


def dotg(a,b,ca,cb):
    return lax.dot_general(a,b,(((ca,),(cb,)),((),())),preferred_element_type=f32)


def dot3(a,b,ca=1,cb=0):
    ah,al=split(a); bh,bl=split(b)
    return dotg(ah,bh,ca,cb)+(dotg(ah,bl,ca,cb)+dotg(al,bh,ca,cb))


def inverse_root(m, c, pv):
    n = m.shape[0]
    lane = lax.broadcasted_iota(jnp.int32, (8, n), 1)
    sub = lax.broadcasted_iota(jnp.int32, (8, n), 0)

    def step(o, piv):
        k0 = pl.multiple_of(o * 8, 8)
        block = m[pl.ds(k0, 8), :]
        for k in range(8):
            pv[k] = jnp.take_along_axis(block, jnp.full((8, n), k0 + k, jnp.int32), axis=1)
        rows = [jnp.broadcast_to(m[pl.ds(k0 + k, 1), :], (8, n)) for k in range(8)]
        s = [[None] * 8 for _ in range(8)]
        for k in range(8):
            for i in range(k + 1):
                s[i][k] = jnp.broadcast_to(pv[k, i : i + 1, :], (8, n))
        for k in range(8):
            c[k] = jnp.take_along_axis(m[...], jnp.full((n, n), k0 + k, jnp.int32), axis=1)
        mult = [[None] * 8 for _ in range(8)]
        inv = [None] * 8
        for k in range(8):
            inv[k] = 1.0 / s[k][k]
            piv = jnp.where(lane == k0 + k, s[k][k], piv)
            for j in range(k + 1, 8):
                mult[k][j] = s[k][j] * inv[k]
            for i in range(k + 1, 8):
                for j in range(i, 8):
                    s[i][j] = s[i][j] - mult[k][i] * s[k][j]
            for j in range(k + 1, 8):
                rows[j] = rows[j] - mult[k][j] * rows[k]
        after = lane > k0 + 7
        r = [jnp.where(after, rows[k] * inv[k], jnp.where(lane == k0 + k, -1.0, 0.0)) for k in range(8)]
        for i in range(6, -1, -1):
            for k in range(7, i, -1):
                r[i] = r[i] - mult[i][k] * r[k]
        inside = (lane >= k0) & (lane < k0 + 8)
        for b in range(0, n, 8):
            new = jnp.where(inside, 0.0, m[b : b + 8, :])
            for k in range(8):
                new = new - c[k, b : b + 8, :] * r[k]
            m[b : b + 8, :] = new
        own = -r[0]
        for k in range(1, 8):
            own = jnp.where(sub == k, -r[k], own)
        m[pl.ds(k0, 8), :] = own
        return piv

    return lax.fori_loop(0, n // 8, step, jnp.ones((8, n), f32))


def invert_block(s,m,t,c,pv):
    h=s.shape[0]//2
    m[...]=s[:h,:h]
    piv=inverse_root(m,c,pv)
    t1=m[...]*lax.rsqrt(piv[0:1,:])
    low=dot3(s[h:,:h],t1)
    m[...]=s[h:,h:]-dot3(low,low,1,1)
    piv=inverse_root(m,c,pv)
    t2=m[...]*lax.rsqrt(piv[0:1,:])
    t[:h,:h]=t1
    t[h:,h:]=t2
    t[h:,:h]=jnp.zeros((h,h),f32)
    t[:h,h:]=-dot3(t1,dot3(low,t2,0,0))


BLOCK = 256
GROUPS = (0, 1, 3)


def panel_groups(count):
    ends = GROUPS[1:] + (count,)
    return [range(a, min(b, count)) for a, b in zip(GROUPS, ends) if a < count]


def group_blocks(groups, count, devices):
    listed, late = [], []
    for panels in groups:
        blocks = late + [(i, p) for p in panels for i in range(p, count)]
        late = []
        if panels[-1] + 2 < count and len(blocks) % devices == 1:
            late = [blocks.pop()]
        listed.append((blocks, late))
    return listed


def place_units(blocks, devices):
    size = -(-len(blocks) // devices)
    blocks = blocks + [blocks[-1]] * (size * devices - len(blocks))
    held = [blocks[d * size : (d + 1) * size] for d in range(devices)]
    where = {}
    for k, block in enumerate(blocks):
        where.setdefault(block, (k // size, k % size))
    return size, held, where


def fetch(band, pieces, buf, sem):
    copies = []
    for r, parts in enumerate(pieces):
        first = 0
        for part in parts:
            dst = buf.at[band ^ r, pl.ds(first, part.shape[0])]
            copies.append(pltpu.make_async_copy(part, dst, sem.at[len(copies)]))
            first += part.shape[0]
    for copy in copies:
        copy.start()
    for copy in copies:
        copy.wait()


def metric_kernel(scale, counts, with_rows, where, ids, weights, coefs, *refs):
    parts = sum(counts)
    flat, refs = refs[:parts], refs[parts:]
    pieces, at = [], 0
    for c in counts:
        pieces.append(flat[at : at + c])
        at += c
    outs, (mine, high, low, whigh, wlow, sem) = refs[:-6], refs[-6:]
    band = where[0]
    fetch(band, pieces, mine, sem)
    width = mine.shape[2]
    for j in range(mine.shape[0]):
        cols = slice(j * width, (j + 1) * width)
        corr = jnp.dot(weights[...], mine[j], preferred_element_type=f32)
        weighted = dot3(coefs[...], corr) * (1.0 / scale)
        high[:, cols], low[:, cols] = split(corr)
        whigh[:, cols], wlow[:, cols] = split(weighted)
    if with_rows:
        rows = outs[-1]
        outs = outs[:-1]
        height = rows.shape[0]
        for j in range(mine.shape[0]):
            own = pl.ds(pl.multiple_of(band * height, height), height)
            rows[:, j * width : (j + 1) * width] = mine[j, own, :]
    first = 0
    for out in outs:
        slabs, size, part, _ = out.shape

        def one(n, _, first=first, out=out, slabs=slabs, part=part):
            i, p = ids[first + n, 0], ids[first + n, 1]
            rows = pl.ds(pl.multiple_of(i * BLOCK, BLOCK), BLOCK)
            cols = pl.ds(pl.multiple_of(p * BLOCK, BLOCK), BLOCK)
            per = width // BLOCK
            left = mine[i // per, :, pl.ds(pl.multiple_of((i % per) * BLOCK, BLOCK), BLOCK)]
            right = mine[p // per, :, pl.ds(pl.multiple_of((p % per) * BLOCK, BLOCK), BLOCK)]
            total = dotg(left, right, 0, 0)
            paw = dotg(whigh[:, rows], high[:, cols], 0, 0)
            paw = paw + dotg(whigh[:, rows], low[:, cols], 0, 0)
            paw = paw + dotg(wlow[:, rows], high[:, cols], 0, 0)
            out[:, n] = ((total + paw) * scale).reshape(slabs, part, BLOCK)
            return 0

        lax.fori_loop(0, size, one, 0)
        first += size


def metric_units(band, ids, sizes, slabs, weights, coefs, pieces, scale, height):
    bands = sum(p[0].shape[1] for p in pieces)
    grid_rows = sum(part.shape[0] for part in pieces[0])
    terms = weights.shape[0]
    vmem = pl.BlockSpec(memory_space=pltpu.VMEM)
    smem = pl.BlockSpec(memory_space=pltpu.SMEM)
    hbm = pl.BlockSpec(memory_space=pl.ANY)
    flat = [part for p in pieces for part in p]
    outs = [jax.ShapeDtypeStruct((slabs, n, BLOCK // slabs, BLOCK), f32) for n in sizes]
    if height:
        outs.append(jax.ShapeDtypeStruct((height, bands), bf16))
    return pl.pallas_call(
        functools.partial(metric_kernel, scale, [len(p) for p in pieces], bool(height)),
        out_shape=outs,
        in_specs=[smem, smem, vmem, vmem] + [hbm] * len(flat),
        out_specs=[vmem] * len(outs),
        scratch_shapes=[pltpu.VMEM((len(pieces), grid_rows, bands // len(pieces)), bf16)]
        + [pltpu.VMEM((terms, bands), bf16)] * 4
        + [pltpu.SemaphoreType.DMA((len(flat),))],
        compiler_params=pltpu.CompilerParams(vmem_limit_bytes=28 * 2**20),
        cost_estimate=pl.CostEstimate(flops=sum(sizes) * 2 * grid_rows * BLOCK * BLOCK, bytes_accessed=2**23, transcendentals=0),
        name="metric_units",
    )(band, ids, weights, coefs, *flat)


def lead_kernel(scale, own, lead, weights, coefs, out, high, low, whigh, wlow):
    slabs, size, part, _ = out.shape
    corr = jnp.dot(weights[...], own[...], preferred_element_type=f32)
    whigh[...], wlow[...] = split(dot3(coefs[...], corr) * (1.0 / scale))
    high[...], low[...] = split(jnp.dot(weights[...], lead[...], preferred_element_type=f32))
    for n in range(size):
        rows = slice(n * BLOCK, (n + 1) * BLOCK)
        total = dotg(own[:, rows], lead[...], 0, 0)
        paw = dotg(whigh[:, rows], high[...], 0, 0)
        paw = paw + dotg(whigh[:, rows], low[...], 0, 0)
        paw = paw + dotg(wlow[:, rows], high[...], 0, 0)
        out[:, n] = ((total + paw) * scale).reshape(slabs, part, BLOCK)


def lead_units(slabs, weights, coefs, own, lead, scale):
    rows, width = own.shape
    terms = weights.shape[0]
    size = width // BLOCK
    vmem = pl.BlockSpec(memory_space=pltpu.VMEM)
    return pl.pallas_call(
        functools.partial(lead_kernel, scale),
        out_shape=jax.ShapeDtypeStruct((slabs, size, BLOCK // slabs, BLOCK), f32),
        in_specs=[vmem] * 4,
        out_specs=vmem,
        scratch_shapes=[pltpu.VMEM((terms, BLOCK), bf16)] * 2 + [pltpu.VMEM((terms, width), bf16)] * 2,
        compiler_params=pltpu.CompilerParams(vmem_limit_bytes=40 * 2**20),
        cost_estimate=pl.CostEstimate(flops=2 * rows * width * BLOCK, bytes_accessed=2**22, transcendentals=0),
        name="lead_units",
    )(own, lead, weights, coefs)


def spread_lead(value, index, size):
    held = jnp.where(index == 0, value, jnp.zeros_like(value))
    bit = size // 2
    while bit:
        pairs = [(d, d | bit) for d in range(0, size, 2 * bit)]
        got = lax.ppermute(held, "band", pairs)
        held = jnp.where(index & bit == 0, held, got)
        bit //= 2
    return held


def sum_kernel(got, out):
    total = got[0]
    for g in range(1, got.shape[0]):
        total = total + got[g]
    for g in range(out.shape[0]):
        out[g] = total


def sum_units(got):
    return pl.pallas_call(
        sum_kernel,
        out_shape=jax.ShapeDtypeStruct(got.shape, f32),
        in_specs=[pl.BlockSpec(memory_space=pltpu.VMEM)],
        out_specs=pl.BlockSpec(memory_space=pltpu.VMEM),
        name="sum_units",
    )(got)


def group_kernel(panels, npieces, earlier, last, owed, owing, where, spots, *refs):
    pieces = [[r] for r in refs[:npieces]]
    o_ref = refs[npieces]
    refs = refs[npieces + 1 :]
    olds = [refs[3 * q : 3 * q + 3] for q in range(earlier)]
    refs = refs[3 * earlier :]
    if owed:
        t_old, refs = refs[0], refs[1:]
    nout = (1 if last else 3) + owing
    outs, (buf, m, t, s, c, pv, sem) = refs[:nout], refs[nout : nout + 7]
    if owing:
        t_out, outs = outs[-1], outs[:-1]
    if owed:
        refs, (h_old, l_old) = refs[:-2], refs[-2:]
    if last:
        y_out, (hi, lo) = outs[0], refs[nout + 7 :]
        base = panels[0] * BLOCK
        for q, (oh, ol, oy) in enumerate(olds):
            begin = sum(olds[k][2].shape[1] for k in range(q))
            y_out[:, begin : begin + oy.shape[1]] = oy[...]
    else:
        hi, lo, y_out = outs
        base = 0
    fetch(where[0], pieces, buf, sem)
    count = o_ref.shape[1] // BLOCK
    height = o_ref.shape[0]
    first = 0

    def block(k):
        return buf[spots[k, 0], :, spots[k, 1]].reshape(BLOCK, BLOCK)

    if owed:
        end = slice((count - 1) * BLOCK, count * BLOCK)
        used = slice(panels[0] * BLOCK, (count - 1) * BLOCK)
        before = slice((panels[0] - 1) * BLOCK, panels[0] * BLOCK)
        h_old[used, :] = olds[-1][0][used, :]
        l_old[used, :] = olds[-1][1][used, :]
        x = block(0)
        for h, l, _ in olds[:-1]:
            x = x - dotg(h[end, :], h[before, :], 1, 1)
            x = x - (dotg(h[end, :], l[before, :], 1, 1) + dotg(l[end, :], h[before, :], 1, 1))
        h_old[end, :], l_old[end, :] = split(dot3(x, t_old[...]))
        olds = list(olds[:-1]) + [(h_old, l_old, olds[-1][2])]
        first = 1

    for step, p in enumerate(panels):
        K = step * BLOCK
        mine = slice(K, K + BLOCK)
        cp = slice(p * BLOCK, (p + 1) * BLOCK)
        stores = [(oh, ol, oy, oy.shape[1], 0) for oh, ol, oy in olds] + ([(hi, lo, y_out, K, base)] if K else [])

        def reduce_block(i, x):
            ri = pl.ds(pl.multiple_of(i * BLOCK, BLOCK), BLOCK)
            for h, l, _, k, _b in stores:
                x = x - dotg(h[ri, :k], h[cp, :k], 1, 1)
                x = x - (dotg(h[ri, :k], l[cp, :k], 1, 1) + dotg(l[ri, :k], h[cp, :k], 1, 1))
            return x

        s[...] = reduce_block(p, block(first))
        invert_block(s[...], m, t, c, pv)
        th, tl = split(t[...])

        def rows_below(n, _):
            i = p + 1 + n
            xh, xl = split(reduce_block(i, block(first + 1 + n)))
            r = dotg(xh, th, 1, 0) + (dotg(xh, tl, 1, 0) + dotg(xl, th, 1, 0))
            ri = pl.ds(pl.multiple_of(i * BLOCK, BLOCK), BLOCK)
            hi[ri, mine], lo[ri, mine] = split(r)
            return 0

        lax.fori_loop(0, count - 1 - p - owing, rows_below, 0)

        def rows_orbital(n, _):
            ri = pl.ds(pl.multiple_of(n * BLOCK, BLOCK), BLOCK)
            x = o_ref[ri, cp].astype(f32)
            for h, _l, y, k, b in stores:
                x = x - dotg(y[ri, b : b + k], h[cp, :k], 1, 1)
            xh, xl = split(x)
            r = dotg(xh, th, 1, 0) + (dotg(xh, tl, 1, 0) + dotg(xl, th, 1, 0))
            y_out[ri, base + K : base + K + BLOCK] = r.astype(bf16)
            return 0

        lax.fori_loop(0, height // BLOCK, rows_orbital, 0)
        first += count - p
    if owing:
        t_out[...] = t[...]


def solve_group(panels, band, spots, pieces, rows, olds, t_old, owing):
    height, bands = rows.shape
    width = len(panels) * BLOCK
    last = panels[-1] + 1 == bands // BLOCK
    flat = [x for old in olds for x in old]
    vmem = pl.BlockSpec(memory_space=pltpu.VMEM)
    smem = pl.BlockSpec(memory_space=pltpu.SMEM)
    if last:
        outs = [jax.ShapeDtypeStruct((height, bands), bf16)]
        more = [pltpu.VMEM((bands, width), bf16)] * 2
    else:
        outs = [jax.ShapeDtypeStruct((bands, width), bf16)] * 2 + [jax.ShapeDtypeStruct((height, width), bf16)]
        more = []
    if owing:
        outs.append(jax.ShapeDtypeStruct((BLOCK, BLOCK), f32))
    if t_old is not None:
        flat.append(t_old)
        more = more + [pltpu.VMEM((bands, BLOCK), bf16)] * 2
    flops = len(panels) * 10 * 10**9
    return pl.pallas_call(
        functools.partial(group_kernel, list(panels), len(pieces), len(olds), last, t_old is not None, owing),
        out_shape=outs,
        in_specs=[smem, smem] + [pl.BlockSpec(memory_space=pl.ANY)] * len(pieces) + [vmem] * (1 + len(flat)),
        out_specs=[vmem] * len(outs),
        scratch_shapes=[
            pltpu.VMEM((len(pieces),) + pieces[0].shape, f32),
            pltpu.VMEM((BLOCK // 2, BLOCK // 2), f32),
            pltpu.VMEM((BLOCK, BLOCK), f32),
            pltpu.VMEM((BLOCK, BLOCK), f32),
            pltpu.VMEM((8, BLOCK // 2, BLOCK // 2), f32),
            pltpu.VMEM((8, 8, BLOCK // 2), f32),
            pltpu.SemaphoreType.DMA((len(pieces),)),
        ]
        + more,
        compiler_params=pltpu.CompilerParams(vmem_limit_bytes=36 * 2**20),
        cost_estimate=pl.CostEstimate(flops=flops, bytes_accessed=2**23, transcendentals=0),
        name="solve_group",
    )(band, spots, *pieces, rows, *flat)


def gather_bands(parts, size):
    held = {0: list(parts)}
    bit = size // 2
    while bit:
        swap = [(d, d ^ bit) for d in range(size)]
        for r in list(held):
            got = []
            for x in held[r]:
                got.append(lax.ppermute(x, "band", swap))
            held[r | bit] = got
        bit //= 2
    return [held[r] for r in range(size)]


def atom_rows(projectors, sphere_start, proj_count, owner_slab, correlation_coef, height):
    slabs = lax.axis_size("grid")
    atoms, most, span = projectors.shape
    per_slab = atoms // slabs
    owned = owner_slab == lax.axis_index("grid")
    rank = jnp.cumsum(owned.astype(jnp.int32)) - 1
    pick = owned[None, :] & (rank[None, :] == jnp.arange(per_slab, dtype=jnp.int32)[:, None])

    def choose(values):
        shaped = pick.reshape(pick.shape + (1,) * (values.ndim - 1))
        return jnp.sum(jnp.where(shaped, values[None], jnp.zeros_like(values)[None]), axis=1, dtype=values.dtype)

    weights = choose(projectors)
    active = jnp.arange(most)[None, :] < choose(proj_count)[:, None]
    block = choose(sphere_start) // span
    spots = (block[:, None] == jnp.arange(height // span)[None, :])[:, None, :, None] & active[:, :, None, None]
    rows = jnp.where(spots, weights[:, :, None, :], jnp.zeros_like(weights)[:, :, None, :])
    coefs = choose(correlation_coef)
    same = jnp.eye(per_slab, dtype=bool)[:, None, :, None]
    square = jnp.where(same, coefs[:, :, None, :], 0.0)
    return rows.reshape(per_slab * most, height), square.reshape(per_slab * most, per_slab * most)


def shards(orbitals, projectors, sphere_start, proj_count, owner_slab, correlation_coef):
    slabs, devices = lax.axis_size("grid"), lax.axis_size("band")
    grid_rows, width = orbitals.shape
    scale = 1.0 / (grid_rows * slabs)
    height = grid_rows // devices
    count = width * devices // BLOCK
    band_index = lax.axis_index("band")
    band = band_index.reshape(1)
    half = grid_rows // 2
    lead = spread_lead(orbitals[:, :BLOCK], band_index, devices)
    pieces = gather_bands([orbitals[:half], orbitals[half:]], devices)
    pieces[0] = [orbitals]
    weights, coefs = atom_rows(projectors, sphere_start, proj_count, owner_slab, correlation_coef, grid_rows)

    groups = panel_groups(count)
    listed = group_blocks(groups, count, devices)
    plans = [place_units(blocks, devices) for blocks, _ in listed]
    tables = [jnp.asarray(held, jnp.int32)[band_index] for _, held, _ in plans]
    assert plans[0][0] == width // BLOCK
    sizes = [size for size, _, _ in plans]
    first = lead_units(slabs, weights, coefs, orbitals, lead, scale)
    second, rows = metric_units(band, tables[1], sizes[1:2], slabs, weights, coefs, pieces, scale, height)
    ids = jnp.concatenate(tables[2:])
    rest = metric_units(band, ids, sizes[2:], slabs, weights, coefs, pieces, scale, 0)
    olds, t_old, late = [], None, []
    for g, (panels, (_, _, where), units) in enumerate(zip(groups, plans, [first, second] + list(rest))):
        got = lax.all_to_all(units, "grid", split_axis=0, concat_axis=0, tiled=True)
        part = sum_units(got)
        part = lax.all_to_all(part, "grid", split_axis=0, concat_axis=0, tiled=True)
        all_parts = [x[0] for x in gather_bands([part], devices)]
        runs = [list(panels)] if panels[-1] + 1 == count else [[p] for p in panels]
        for run in runs:
            order = [where[block] for block in late]
            missing = listed[g][1] if run[-1] == panels[-1] else []
            order += [where[i, p] for p in run for i in range(p, count) if (i, p) not in missing]
            spots = jnp.asarray(order, jnp.int32)
            got = solve_group(run, band, spots, all_parts, rows, olds, t_old, len(missing))
            late, t_old = [], None
            if missing:
                late, t_old = missing, got[-1]
                got = got[:-1]
            olds.append(got)
    return olds[-1][0]


def solution(mesh):
    in_specs = (P("grid", "band"), P(), P(), P(), P(), P())
    out_specs = P(("grid", "band"), None)
    return jax.shard_map(shards, mesh=mesh, in_specs=in_specs, out_specs=out_specs, check_vma=False)
```

```python
import functools

import jax, jax.numpy as jnp
from jax import lax
from jax.experimental import pallas as pl
from jax.experimental.pallas import tpu as pltpu
from jax.sharding import PartitionSpec as P


f32,bf16=jnp.float32,jnp.bfloat16


def split(x):
    hi=x.astype(bf16)
    return hi,(x-hi.astype(f32)).astype(bf16)


def dotg(a,b,ca,cb):
    return lax.dot_general(a,b,(((ca,),(cb,)),((),())),preferred_element_type=f32)


def dot3(a,b,ca=1,cb=0):
    ah,al=split(a); bh,bl=split(b)
    return dotg(ah,bh,ca,cb)+(dotg(ah,bl,ca,cb)+dotg(al,bh,ca,cb))


def inverse_root(m, c, pv):
    n = m.shape[0]
    lane = lax.broadcasted_iota(jnp.int32, (8, n), 1)
    sub = lax.broadcasted_iota(jnp.int32, (8, n), 0)

    def step(o, piv):
        k0 = pl.multiple_of(o * 8, 8)
        block = m[pl.ds(k0, 8), :]
        for k in range(8):
            pv[k] = jnp.take_along_axis(block, jnp.full((8, n), k0 + k, jnp.int32), axis=1)
        rows = [jnp.broadcast_to(m[pl.ds(k0 + k, 1), :], (8, n)) for k in range(8)]
        s = [[None] * 8 for _ in range(8)]
        for k in range(8):
            for i in range(k + 1):
                s[i][k] = jnp.broadcast_to(pv[k, i : i + 1, :], (8, n))
        for k in range(8):
            c[k] = jnp.take_along_axis(m[...], jnp.full((n, n), k0 + k, jnp.int32), axis=1)
        mult = [[None] * 8 for _ in range(8)]
        inv = [None] * 8
        for k in range(8):
            inv[k] = 1.0 / s[k][k]
            piv = jnp.where(lane == k0 + k, s[k][k], piv)
            for j in range(k + 1, 8):
                mult[k][j] = s[k][j] * inv[k]
            for i in range(k + 1, 8):
                for j in range(i, 8):
                    s[i][j] = s[i][j] - mult[k][i] * s[k][j]
            for j in range(k + 1, 8):
                rows[j] = rows[j] - mult[k][j] * rows[k]
        after = lane > k0 + 7
        r = [jnp.where(after, rows[k] * inv[k], jnp.where(lane == k0 + k, -1.0, 0.0)) for k in range(8)]
        for i in range(6, -1, -1):
            for k in range(7, i, -1):
                r[i] = r[i] - mult[i][k] * r[k]
        inside = (lane >= k0) & (lane < k0 + 8)
        for b in range(0, n, 8):
            new = jnp.where(inside, 0.0, m[b : b + 8, :])
            for k in range(8):
                new = new - c[k, b : b + 8, :] * r[k]
            m[b : b + 8, :] = new
        own = -r[0]
        for k in range(1, 8):
            own = jnp.where(sub == k, -r[k], own)
        m[pl.ds(k0, 8), :] = own
        return piv

    return lax.fori_loop(0, n // 8, step, jnp.ones((8, n), f32))


def invert_block(s,m,t,c,pv):
    h=s.shape[0]//2
    m[...]=s[:h,:h]
    piv=inverse_root(m,c,pv)
    t1=m[...]*lax.rsqrt(piv[0:1,:])
    low=dot3(s[h:,:h],t1)
    m[...]=s[h:,h:]-dot3(low,low,1,1)
    piv=inverse_root(m,c,pv)
    t2=m[...]*lax.rsqrt(piv[0:1,:])
    t[:h,:h]=t1
    t[h:,h:]=t2
    t[h:,:h]=jnp.zeros((h,h),f32)
    t[:h,h:]=-dot3(t1,dot3(low,t2,0,0))


BLOCK = 256
GROUPS = (0, 1, 3)


def panel_groups(count):
    ends = GROUPS[1:] + (count,)
    return [range(a, min(b, count)) for a, b in zip(GROUPS, ends) if a < count]


def group_blocks(groups, count, devices):
    listed, late = [], []
    for panels in groups:
        blocks = late + [(i, p) for p in panels for i in range(p, count)]
        late = []
        if panels[-1] + 2 < count and len(blocks) % devices == 1:
            late = [blocks.pop()]
        listed.append((blocks, late))
    return listed


def place_units(blocks, devices):
    size = -(-len(blocks) // devices)
    blocks = blocks + [blocks[-1]] * (size * devices - len(blocks))
    held = [blocks[d * size : (d + 1) * size] for d in range(devices)]
    where = {}
    for k, block in enumerate(blocks):
        where.setdefault(block, (k // size, k % size))
    return size, held, where


def fetch(band, pieces, buf, sem):
    copies = []
    for r, parts in enumerate(pieces):
        first = 0
        for part in parts:
            dst = buf.at[band ^ r, pl.ds(first, part.shape[0])]
            copies.append(pltpu.make_async_copy(part, dst, sem.at[len(copies)]))
            first += part.shape[0]
    for copy in copies:
        copy.start()
    for copy in copies:
        copy.wait()


def metric_kernel(scale, counts, with_rows, where, ids, weights, coefs, *refs):
    parts = sum(counts)
    flat, refs = refs[:parts], refs[parts:]
    pieces, at = [], 0
    for c in counts:
        pieces.append(flat[at : at + c])
        at += c
    outs, (mine, high, low, whigh, wlow, sem) = refs[:-6], refs[-6:]
    band = where[0]
    fetch(band, pieces, mine, sem)
    width = mine.shape[2]
    for j in range(mine.shape[0]):
        cols = slice(j * width, (j + 1) * width)
        corr = jnp.dot(weights[...], mine[j], preferred_element_type=f32)
        weighted = dot3(coefs[...], corr) * (1.0 / scale)
        high[:, cols], low[:, cols] = split(corr)
        whigh[:, cols], wlow[:, cols] = split(weighted)
    if with_rows:
        rows = outs[-1]
        outs = outs[:-1]
        height = rows.shape[0]
        for j in range(mine.shape[0]):
            own = pl.ds(pl.multiple_of(band * height, height), height)
            rows[:, j * width : (j + 1) * width] = mine[j, own, :]
    first = 0
    for out in outs:
        slabs, size, part, _ = out.shape

        def one(n, _, first=first, out=out, slabs=slabs, part=part):
            i, p = ids[first + n, 0], ids[first + n, 1]
            rows = pl.ds(pl.multiple_of(i * BLOCK, BLOCK), BLOCK)
            cols = pl.ds(pl.multiple_of(p * BLOCK, BLOCK), BLOCK)
            per = width // BLOCK
            left = mine[i // per, :, pl.ds(pl.multiple_of((i % per) * BLOCK, BLOCK), BLOCK)]
            right = mine[p // per, :, pl.ds(pl.multiple_of((p % per) * BLOCK, BLOCK), BLOCK)]
            total = dotg(left, right, 0, 0)
            paw = dotg(whigh[:, rows], high[:, cols], 0, 0)
            paw = paw + dotg(whigh[:, rows], low[:, cols], 0, 0)
            paw = paw + dotg(wlow[:, rows], high[:, cols], 0, 0)
            out[:, n] = ((total + paw) * scale).reshape(slabs, part, BLOCK)
            return 0

        lax.fori_loop(0, size, one, 0)
        first += size


def metric_units(band, ids, sizes, slabs, weights, coefs, pieces, scale, height):
    bands = sum(p[0].shape[1] for p in pieces)
    grid_rows = sum(part.shape[0] for part in pieces[0])
    terms = weights.shape[0]
    vmem = pl.BlockSpec(memory_space=pltpu.VMEM)
    smem = pl.BlockSpec(memory_space=pltpu.SMEM)
    hbm = pl.BlockSpec(memory_space=pl.ANY)
    flat = [part for p in pieces for part in p]
    outs = [jax.ShapeDtypeStruct((slabs, n, BLOCK // slabs, BLOCK), f32) for n in sizes]
    if height:
        outs.append(jax.ShapeDtypeStruct((height, bands), bf16))
    return pl.pallas_call(
        functools.partial(metric_kernel, scale, [len(p) for p in pieces], bool(height)),
        out_shape=outs,
        in_specs=[smem, smem, vmem, vmem] + [hbm] * len(flat),
        out_specs=[vmem] * len(outs),
        scratch_shapes=[pltpu.VMEM((len(pieces), grid_rows, bands // len(pieces)), bf16)]
        + [pltpu.VMEM((terms, bands), bf16)] * 4
        + [pltpu.SemaphoreType.DMA((len(flat),))],
        compiler_params=pltpu.CompilerParams(vmem_limit_bytes=28 * 2**20),
        cost_estimate=pl.CostEstimate(flops=sum(sizes) * 2 * grid_rows * BLOCK * BLOCK, bytes_accessed=2**23, transcendentals=0),
        name="metric_units",
    )(band, ids, weights, coefs, *flat)


def lead_kernel(scale, own, lead, weights, coefs, out, high, low, whigh, wlow):
    slabs, size, part, _ = out.shape
    corr = jnp.dot(weights[...], own[...], preferred_element_type=f32)
    whigh[...], wlow[...] = split(dot3(coefs[...], corr) * (1.0 / scale))
    high[...], low[...] = split(jnp.dot(weights[...], lead[...], preferred_element_type=f32))
    for n in range(size):
        rows = slice(n * BLOCK, (n + 1) * BLOCK)
        total = dotg(own[:, rows], lead[...], 0, 0)
        paw = dotg(whigh[:, rows], high[...], 0, 0)
        paw = paw + dotg(whigh[:, rows], low[...], 0, 0)
        paw = paw + dotg(wlow[:, rows], high[...], 0, 0)
        out[:, n] = ((total + paw) * scale).reshape(slabs, part, BLOCK)


def lead_units(slabs, weights, coefs, own, lead, scale):
    rows, width = own.shape
    terms = weights.shape[0]
    size = width // BLOCK
    vmem = pl.BlockSpec(memory_space=pltpu.VMEM)
    return pl.pallas_call(
        functools.partial(lead_kernel, scale),
        out_shape=jax.ShapeDtypeStruct((slabs, size, BLOCK // slabs, BLOCK), f32),
        in_specs=[vmem] * 4,
        out_specs=vmem,
        scratch_shapes=[pltpu.VMEM((terms, BLOCK), bf16)] * 2 + [pltpu.VMEM((terms, width), bf16)] * 2,
        compiler_params=pltpu.CompilerParams(vmem_limit_bytes=40 * 2**20),
        cost_estimate=pl.CostEstimate(flops=2 * rows * width * BLOCK, bytes_accessed=2**22, transcendentals=0),
        name="lead_units",
    )(own, lead, weights, coefs)


def spread_lead(value, index, size):
    held = jnp.where(index == 0, value, jnp.zeros_like(value))
    bit = size // 2
    while bit:
        pairs = [(d, d | bit) for d in range(0, size, 2 * bit)]
        got = lax.ppermute(held, "band", pairs)
        held = jnp.where(index & bit == 0, held, got)
        bit //= 2
    return held


def sum_kernel(got, out):
    total = got[0]
    for g in range(1, got.shape[0]):
        total = total + got[g]
    for g in range(out.shape[0]):
        out[g] = total


def sum_units(got):
    return pl.pallas_call(
        sum_kernel,
        out_shape=jax.ShapeDtypeStruct(got.shape, f32),
        in_specs=[pl.BlockSpec(memory_space=pltpu.VMEM)],
        out_specs=pl.BlockSpec(memory_space=pltpu.VMEM),
        name="sum_units",
    )(got)


def group_kernel(panels, npieces, earlier, last, owed, owing, where, spots, *refs):
    pieces = [[r] for r in refs[:npieces]]
    o_ref = refs[npieces]
    refs = refs[npieces + 1 :]
    olds = [refs[3 * q : 3 * q + 3] for q in range(earlier)]
    refs = refs[3 * earlier :]
    if owed:
        t_old, refs = refs[0], refs[1:]
    nout = (1 if last else 3) + owing
    outs, (buf, m, t, s, c, pv, sem) = refs[:nout], refs[nout : nout + 7]
    if owing:
        t_out, outs = outs[-1], outs[:-1]
    if owed:
        refs, (h_old, l_old) = refs[:-2], refs[-2:]
    if last:
        y_out, (hi, lo) = outs[0], refs[nout + 7 :]
        base = panels[0] * BLOCK
        for q, (oh, ol, oy) in enumerate(olds):
            begin = sum(olds[k][2].shape[1] for k in range(q))
            y_out[:, begin : begin + oy.shape[1]] = oy[...]
    else:
        hi, lo, y_out = outs
        base = 0
    fetch(where[0], pieces, buf, sem)
    count = o_ref.shape[1] // BLOCK
    first = 0

    def block(k):
        return buf[spots[k, 0], :, spots[k, 1]].reshape(BLOCK, BLOCK)

    if owed:
        end = slice((count - 1) * BLOCK, count * BLOCK)
        used = slice(panels[0] * BLOCK, (count - 1) * BLOCK)
        before = slice((panels[0] - 1) * BLOCK, panels[0] * BLOCK)
        h_old[used, :] = olds[-1][0][used, :]
        l_old[used, :] = olds[-1][1][used, :]
        x = block(0)
        for h, l, _ in olds[:-1]:
            x = x - dotg(h[end, :], h[before, :], 1, 1)
            x = x - (dotg(h[end, :], l[before, :], 1, 1) + dotg(l[end, :], h[before, :], 1, 1))
        h_old[end, :], l_old[end, :] = split(dot3(x, t_old[...]))
        olds = list(olds[:-1]) + [(h_old, l_old, olds[-1][2])]
        first = 1

    for step, p in enumerate(panels):
        K = step * BLOCK
        mine = slice(K, K + BLOCK)
        cp = slice(p * BLOCK, (p + 1) * BLOCK)
        stores = [(oh, ol, oy, oy.shape[1], 0) for oh, ol, oy in olds] + ([(hi, lo, y_out, K, base)] if K else [])

        def reduce_rows(ri, x):
            for h, l, _, k, _b in stores:
                x = x - dotg(h[ri, :k], h[cp, :k], 1, 1)
                x = x - (dotg(h[ri, :k], l[cp, :k], 1, 1) + dotg(l[ri, :k], h[cp, :k], 1, 1))
            return x

        s[...] = reduce_rows(cp, block(first))
        invert_block(s[...], m, t, c, pv)
        th, tl = split(t[...])

        def rows_below(n, high):
            ri = pl.ds(pl.multiple_of((p + 1 + n) * BLOCK, BLOCK), high * BLOCK)
            x = jnp.concatenate([block(first + 1 + n + k) for k in range(high)], axis=0)
            xh, xl = split(reduce_rows(ri, x))
            r = dotg(xh, th, 1, 0) + (dotg(xh, tl, 1, 0) + dotg(xl, th, 1, 0))
            hi[ri, mine], lo[ri, mine] = split(r)

        below = count - 1 - p - owing

        def two_below(n, _):
            rows_below(2 * n, 2)
            return 0

        if below > 1:
            lax.fori_loop(0, below // 2, two_below, 0)
        if below % 2:
            rows_below(below - 1, 1)

        x = o_ref[:, cp].astype(f32)
        for h, _l, y, k, b in stores:
            x = x - dotg(y[:, b : b + k], h[cp, :k], 1, 1)
        xh, xl = split(x)
        r = dotg(xh, th, 1, 0) + (dotg(xh, tl, 1, 0) + dotg(xl, th, 1, 0))
        y_out[:, base + K : base + K + BLOCK] = r.astype(bf16)
        first += count - p
    if owing:
        t_out[...] = t[...]


def solve_group(panels, band, spots, pieces, rows, olds, t_old, owing):
    height, bands = rows.shape
    width = len(panels) * BLOCK
    last = panels[-1] + 1 == bands // BLOCK
    flat = [x for old in olds for x in old]
    vmem = pl.BlockSpec(memory_space=pltpu.VMEM)
    smem = pl.BlockSpec(memory_space=pltpu.SMEM)
    if last:
        outs = [jax.ShapeDtypeStruct((height, bands), bf16)]
        more = [pltpu.VMEM((bands, width), bf16)] * 2
    else:
        outs = [jax.ShapeDtypeStruct((bands, width), bf16)] * 2 + [jax.ShapeDtypeStruct((height, width), bf16)]
        more = []
    if owing:
        outs.append(jax.ShapeDtypeStruct((BLOCK, BLOCK), f32))
    if t_old is not None:
        flat.append(t_old)
        more = more + [pltpu.VMEM((bands, BLOCK), bf16)] * 2
    flops = len(panels) * 10 * 10**9
    return pl.pallas_call(
        functools.partial(group_kernel, list(panels), len(pieces), len(olds), last, t_old is not None, owing),
        out_shape=outs,
        in_specs=[smem, smem] + [pl.BlockSpec(memory_space=pl.ANY)] * len(pieces) + [vmem] * (1 + len(flat)),
        out_specs=[vmem] * len(outs),
        scratch_shapes=[
            pltpu.VMEM((len(pieces),) + pieces[0].shape, f32),
            pltpu.VMEM((BLOCK // 2, BLOCK // 2), f32),
            pltpu.VMEM((BLOCK, BLOCK), f32),
            pltpu.VMEM((BLOCK, BLOCK), f32),
            pltpu.VMEM((8, BLOCK // 2, BLOCK // 2), f32),
            pltpu.VMEM((8, 8, BLOCK // 2), f32),
            pltpu.SemaphoreType.DMA((len(pieces),)),
        ]
        + more,
        compiler_params=pltpu.CompilerParams(vmem_limit_bytes=36 * 2**20),
        cost_estimate=pl.CostEstimate(flops=flops, bytes_accessed=2**23, transcendentals=0),
        name="solve_group",
    )(band, spots, *pieces, rows, *flat)


def gather_bands(parts, size):
    held = {0: list(parts)}
    bit = size // 2
    while bit:
        swap = [(d, d ^ bit) for d in range(size)]
        for r in list(held):
            got = []
            for x in held[r]:
                got.append(lax.ppermute(x, "band", swap))
            held[r | bit] = got
        bit //= 2
    return [held[r] for r in range(size)]


def atom_rows(projectors, sphere_start, proj_count, owner_slab, correlation_coef, height):
    slabs = lax.axis_size("grid")
    atoms, most, span = projectors.shape
    per_slab = atoms // slabs
    owned = owner_slab == lax.axis_index("grid")
    rank = jnp.cumsum(owned.astype(jnp.int32)) - 1
    pick = owned[None, :] & (rank[None, :] == jnp.arange(per_slab, dtype=jnp.int32)[:, None])

    def choose(values):
        shaped = pick.reshape(pick.shape + (1,) * (values.ndim - 1))
        return jnp.sum(jnp.where(shaped, values[None], jnp.zeros_like(values)[None]), axis=1, dtype=values.dtype)

    weights = choose(projectors)
    active = jnp.arange(most)[None, :] < choose(proj_count)[:, None]
    block = choose(sphere_start) // span
    spots = (block[:, None] == jnp.arange(height // span)[None, :])[:, None, :, None] & active[:, :, None, None]
    rows = jnp.where(spots, weights[:, :, None, :], jnp.zeros_like(weights)[:, :, None, :])
    coefs = choose(correlation_coef)
    same = jnp.eye(per_slab, dtype=bool)[:, None, :, None]
    square = jnp.where(same, coefs[:, :, None, :], 0.0)
    return rows.reshape(per_slab * most, height), square.reshape(per_slab * most, per_slab * most)


def shards(orbitals, projectors, sphere_start, proj_count, owner_slab, correlation_coef):
    slabs, devices = lax.axis_size("grid"), lax.axis_size("band")
    grid_rows, width = orbitals.shape
    scale = 1.0 / (grid_rows * slabs)
    height = grid_rows // devices
    count = width * devices // BLOCK
    band_index = lax.axis_index("band")
    band = band_index.reshape(1)
    half = grid_rows // 2
    lead = spread_lead(orbitals[:, :BLOCK], band_index, devices)
    pieces = gather_bands([orbitals[:half], orbitals[half:]], devices)
    pieces[0] = [orbitals]
    weights, coefs = atom_rows(projectors, sphere_start, proj_count, owner_slab, correlation_coef, grid_rows)

    groups = panel_groups(count)
    listed = group_blocks(groups, count, devices)
    plans = [place_units(blocks, devices) for blocks, _ in listed]
    tables = [jnp.asarray(held, jnp.int32)[band_index] for _, held, _ in plans]
    assert plans[0][0] == width // BLOCK
    sizes = [size for size, _, _ in plans]
    first = lead_units(slabs, weights, coefs, orbitals, lead, scale)
    second, rows = metric_units(band, tables[1], sizes[1:2], slabs, weights, coefs, pieces, scale, height)
    ids = jnp.concatenate(tables[2:])
    rest = metric_units(band, ids, sizes[2:], slabs, weights, coefs, pieces, scale, 0)
    olds, t_old, late = [], None, []
    for g, (panels, (_, _, where), units) in enumerate(zip(groups, plans, [first, second] + list(rest))):
        got = lax.all_to_all(units, "grid", split_axis=0, concat_axis=0, tiled=True)
        part = sum_units(got)
        part = lax.all_to_all(part, "grid", split_axis=0, concat_axis=0, tiled=True)
        all_parts = [x[0] for x in gather_bands([part], devices)]
        runs = [list(panels)] if panels[-1] + 1 == count else [[p] for p in panels]
        for run in runs:
            order = [where[block] for block in late]
            missing = listed[g][1] if run[-1] == panels[-1] else []
            order += [where[i, p] for p in run for i in range(p, count) if (i, p) not in missing]
            spots = jnp.asarray(order, jnp.int32)
            got = solve_group(run, band, spots, all_parts, rows, olds, t_old, len(missing))
            late, t_old = [], None
            if missing:
                late, t_old = missing, got[-1]
                got = got[:-1]
            olds.append(got)
    return olds[-1][0]


def solution(mesh):
    in_specs = (P("grid", "band"), P(), P(), P(), P(), P())
    out_specs = P(("grid", "band"), None)
    return jax.shard_map(shards, mesh=mesh, in_specs=in_specs, out_specs=out_specs, check_vma=False)
```
